32 devices in a mesh: pipe: 4 (over z), expert: 4 (over y, x), tensor: 2 (over core).
Axes of the slice: x: 2, y: 2, z: 4, core: 2. Of those that a mesh axis runs over, the one named last changes fastest.
Arguments:
- inputs_prev: bfloat16 [4, 512, 3584], P('pipe', 'expert', 'tensor'), may hold values from -6 to 6
- cotangent_next: bfloat16 [4, 512, 3584], P('pipe', 'expert', 'tensor'), may hold values from -6 to 6
- saved_input: bfloat16 [4, 512, 3584], P('pipe', 'expert', 'tensor'), may hold values from -6 to 6
- expert_ids: int32 [2, 4, 512, 8], P(None, 'pipe', 'expert'), may hold values from 0 to 255, as said below
- keep_mask: int32 [2, 4, 512, 8], P(None, 'pipe', 'expert'), may hold values from 0 to 1, as said below
- slot_pos: int32 [2, 4, 512, 8], P(None, 'pipe', 'expert'), may hold values from 0 to 3, as said below
- weight_q: int32 [2, 4, 512, 8], P(None, 'pipe', 'expert'), may hold values from 1 to 4095
- gate_routed: bfloat16 [4, 4, 3584, 512], P('pipe', 'expert', None, 'tensor'), may hold values from -0.09375 to 0.09375
- up_routed: bfloat16 [4, 4, 3584, 512], P('pipe', 'expert', None, 'tensor'), may hold values from -0.09375 to 0.09375
- down_routed: bfloat16 [4, 4, 512, 3584], P('pipe', 'expert', 'tensor'), may hold values from -0.1875 to 0.1875
- gate_shared: bfloat16 [4, 3584, 1024], P('pipe', None, 'tensor'), may hold values from -0.09375 to 0.09375
- up_shared: bfloat16 [4, 3584, 1024], P('pipe', None, 'tensor'), may hold values from -0.09375 to 0.09375
- down_shared: bfloat16 [4, 1024, 3584], P('pipe', 'tensor'), may hold values from -0.1875 to 0.1875
Outputs:
- out_act: bfloat16 [4, 512, 3584], P('pipe', 'expert', 'tensor')
- in_grad: bfloat16 [4, 512, 3584], P('pipe', 'expert', 'tensor')
The draws below stay inside these ranges and needn't reach their ends.
Inputs may be any that keep to these rules, and one draw needn't show every extreme that they name: `expert_ids`: each row names 8 different experts; in every section and micro-batch one expert below 2 is named by every row. `keep_mask`: 1 only where the expert named is below 2; in one block of 128 rows no expert has more than 4 kept choices, and in every section and micro-batch one expert has exactly 4 in every block. `slot_pos`: kept choices of one block naming the same expert hold different slots; 0 where keep_mask is 0.
All inputs are finite; a program needn't handle non-finite values.
Results may differ from the reference program's by a relative error of at most 0.005.
Values may be sent and summed in bfloat16 or wider, within the bound.
A program may use at most 64 MiB of HBM per device.

```python
import jax
import jax.numpy as jnp
from jax import lax

D = 3584
FE = 1024
FS = 1024
SPECIALIST_COUNT = 256
TOPK = 8
TOK_DEV = 128
SECTIONS = 4
EXPERTS = 2
TOKENS = 512
CAP = 4
N_EXPERT = 4
N_TENSOR = 2


def routing_tables(key):
    base = jax.random.fold_in(key, 29)
    key_score, key_lean, key_force, key_order = jax.random.split(base, 4)
    blocks = TOKENS // TOK_DEV
    choices = TOK_DEV * TOPK
    gating_logits = jax.random.randint(key_score, (2, SECTIONS, TOKENS, SPECIALIST_COUNT), 0, 65536)
    preference_offset = jax.random.randint(key_lean, (SPECIALIST_COUNT,), 0, 3) * 32768
    imposed_selection = jax.random.randint(key_force, (2, SECTIONS, 1, 1), 0, EXPERTS)
    uniform_draws = jnp.arange(SPECIALIST_COUNT, dtype=jnp.int32)
    extra_increment = jnp.where(uniform_draws == imposed_selection, 1 << 20, 0)
    sorted_specialists = (gating_logits + preference_offset + extra_increment) * SPECIALIST_COUNT + uniform_draws
    _, chosen = lax.top_k(sorted_specialists, TOPK)
    chosen = chosen.astype(jnp.int32)
    lined = chosen.reshape(2 * SECTIONS * blocks, choices)
    onehot = (lined[:, :, None] == jnp.arange(EXPERTS, dtype=jnp.int32)).astype(jnp.int32)
    order_keys = jax.random.split(key_order, 2 * SECTIONS * blocks)
    order = jax.vmap(lambda single: jax.random.permutation(single, choices))(order_keys).astype(jnp.int32)
    placed = jnp.take_along_axis(onehot, order[:, :, None], axis=1)
    before = jnp.cumsum(placed, axis=1) - placed
    rank_sorted = jnp.sum(before * placed, axis=-1)
    inverse = jnp.argsort(order, axis=1, stable=True)
    position = jnp.take_along_axis(rank_sorted, inverse, axis=1)
    kept = (lined < EXPERTS) & (position < CAP)
    slots = jnp.where(kept, position, 0)
    target_shape = (2, SECTIONS, TOKENS, TOPK)
    return (chosen, kept.astype(jnp.int32).reshape(target_shape), slots.astype(jnp.int32).reshape(target_shape))


def draw_expert_ids(key, part):
    return routing_tables(key)[0]


def draw_keep_mask(key, part):
    return routing_tables(key)[1]


def draw_slot_pos(key, part):
    return routing_tables(key)[2]


def with_ends(drawn, own_key, low, largest):
    place = [jax.random.randint(jax.random.fold_in(own_key, axis), (), 0, length) for axis, length in enumerate(drawn.shape)]
    main_axis = drawn.shape.index(max(drawn.shape))
    next_to = place[:main_axis] + [(place[main_axis] + 1) % drawn.shape[main_axis]] + place[main_axis + 1:]
    return drawn.at[tuple(place)].set(low).at[tuple(next_to)].set(largest)


def block_scale(stream_key, extent, cuts, smallest, top_value):
    factor_of = 1.0
    for axis_at, blocks in cuts:
        draws = jax.random.uniform(jax.random.fold_in(jax.random.fold_in(stream_key, 6), axis_at), (blocks,), jnp.float32, smallest / len(cuts), top_value / len(cuts))
        factor_of = factor_of * jnp.repeat(jnp.exp(draws), extent[axis_at] // blocks).reshape((-1,) + (1,) * (len(extent) - 1 - axis_at))
    return factor_of


def scatter_about(own_key, dims, width, bound, shards=(), kind=jnp.bfloat16):
    drawn = jax.random.normal(own_key, dims, jnp.float32) * width
    if len(shards) > 0:
        drawn = block_scale(own_key, dims, shards, -0.22, 0.18) * drawn
    return jnp.clip(drawn, min=-bound, max=bound).astype(kind)


def setup_inputs(seed: int = 0) -> dict:
    key_of = jax.random.split(jax.random.key(seed), 14)
    return {
        "inputs_prev": scatter_about(key_of[0], (SECTIONS, TOKENS, D), 1.0, 6.0, ((0, 4), (1, 4), (2, 2))),
        "cotangent_next": scatter_about(key_of[1], (SECTIONS, TOKENS, D), 1.0, 6.0, ((0, 4), (1, 4), (2, 2))),
        "saved_input": scatter_about(key_of[2], (SECTIONS, TOKENS, D), 1.0, 6.0, ((0, 4), (1, 4), (2, 2))),
        "expert_ids": draw_expert_ids(jax.random.fold_in(key_of[13], 71), 0),
        "keep_mask": draw_keep_mask(jax.random.fold_in(key_of[13], 71), 0),
        "slot_pos": draw_slot_pos(jax.random.fold_in(key_of[13], 71), 0),
        "weight_q": with_ends(jax.random.randint(key_of[6], (2, SECTIONS, TOKENS, TOPK), 1, 4096), jax.random.fold_in(key_of[6], 1), 1, 4095).astype(jnp.int32),
        "gate_routed": scatter_about(key_of[7], (SECTIONS, N_EXPERT, D, FE // 2), D ** -0.5, 0.09375, ((0, 4), (1, 4), (3, 2))),
        "up_routed": scatter_about(key_of[8], (SECTIONS, N_EXPERT, D, FE // 2), D ** -0.5, 0.09375, ((0, 4), (1, 4), (3, 2))),
        "down_routed": scatter_about(key_of[9], (SECTIONS, N_EXPERT, FE // 2, D), FE ** -0.5, 0.1875, ((0, 4), (1, 4), (2, 2))),
        "gate_shared": scatter_about(key_of[10], (SECTIONS, D, FS), D ** -0.5, 0.09375, ((0, 4), (2, 2))),
        "up_shared": scatter_about(key_of[11], (SECTIONS, D, FS), D ** -0.5, 0.09375, ((0, 4), (2, 2))),
        "down_shared": scatter_about(key_of[12], (SECTIONS, FS, D), FS ** -0.5, 0.1875, ((0, 4), (1, 2))),
    }


def swish(values):
    return values * jax.nn.sigmoid(values)


def swish_slope(values):
    logistic = jax.nn.sigmoid(values)
    return logistic * (1.0 + values * (1.0 - logistic))


def slot_plan(choice_ids, kept_flags, slot_index, weight_levels, experts_here, capacity):
    total_slots = experts_here * capacity
    target = jnp.where(kept_flags > 0, choice_ids * capacity + slot_index, total_slots).reshape(-1).astype(jnp.int32)
    source = jnp.broadcast_to(jnp.arange(choice_ids.shape[0], dtype=jnp.int32)[:, None], choice_ids.shape).reshape(-1)
    slot_token = jnp.zeros((total_slots,), jnp.int32).at[target].set(source, mode="drop")
    levels = (weight_levels.astype(jnp.float32) / 4096.0).reshape(-1)
    slot_weight = jnp.zeros((total_slots,), jnp.float32).at[target].set(levels, mode="drop")
    slot_live = jnp.zeros((total_slots,), jnp.float32).at[target].set(1.0, mode="drop")
    return slot_token, slot_weight, slot_live


def contract_last(left, right):
    return lax.dot_general(left, right, (((1,), (1,)), ((), ())), preferred_element_type=jnp.float32)


def expert_pass(packed):
    rows_in, rows_saved, rows_cot, gate_w, up_w, down_w = packed
    part_width = FE // (2 * N_TENSOR)
    gate_pre = jnp.dot(rows_in, gate_w, preferred_element_type=jnp.float32)
    up_pre = jnp.dot(rows_in, up_w, preferred_element_type=jnp.float32)
    hidden = (swish(gate_pre) * up_pre).astype(jnp.bfloat16)
    gate_back = jnp.dot(rows_saved, gate_w, preferred_element_type=jnp.float32)
    up_back = jnp.dot(rows_saved, up_w, preferred_element_type=jnp.float32)
    grad_hidden = contract_last(rows_cot, down_w)
    grad_gate = (grad_hidden * up_back * swish_slope(gate_back)).astype(jnp.bfloat16)
    grad_up = (grad_hidden * swish(gate_back)).astype(jnp.bfloat16)
    result = jnp.zeros((rows_in.shape[0], rows_in.shape[1]), jnp.float32)
    grad_rows = jnp.zeros((rows_in.shape[0], rows_in.shape[1]), jnp.float32)
    for group_j in range(FE // part_width):
        lower = group_j * part_width
        upper = lower + part_width
        piece_out = jnp.dot(hidden[:, lower:upper], down_w[lower:upper], preferred_element_type=jnp.float32)
        result = result + piece_out.astype(jnp.bfloat16).astype(jnp.float32)
        piece_grad = contract_last(grad_gate[:, lower:upper], gate_w[:, lower:upper]) + contract_last(grad_up[:, lower:upper], up_w[:, lower:upper])
        grad_rows = grad_rows + piece_grad.astype(jnp.bfloat16).astype(jnp.float32)
    return result, grad_rows


def shared_pass(full_in, full_saved, full_cot, gate_w, up_w, down_w):
    gate_pre = jnp.dot(full_in, gate_w, preferred_element_type=jnp.float32)
    up_pre = jnp.dot(full_in, up_w, preferred_element_type=jnp.float32)
    hidden = (swish(gate_pre) * up_pre).astype(jnp.bfloat16)
    shared_out = jnp.dot(hidden, down_w, preferred_element_type=jnp.float32)
    gate_back = jnp.dot(full_saved, gate_w, preferred_element_type=jnp.float32)
    up_back = jnp.dot(full_saved, up_w, preferred_element_type=jnp.float32)
    grad_hidden = contract_last(full_cot, down_w)
    grad_gate = (grad_hidden * up_back * swish_slope(gate_back)).astype(jnp.bfloat16)
    grad_up = (grad_hidden * swish(gate_back)).astype(jnp.bfloat16)
    shared_grad = contract_last(grad_gate, gate_w) + contract_last(grad_up, up_w)
    return shared_out, shared_grad


def one_section(packed):
    (section_in, section_saved, section_cot, ids_fwd, keep_fwd, slot_fwd, level_fwd, ids_bwd, keep_bwd, slot_bwd, level_bwd,
     gate_section, up_section, down_section, shared_gate, shared_up, shared_down) = packed
    blocks = TOKENS // TOK_DEV
    half_width = FE // 2

    def plan_all(ids_all, keep_all, slot_all, level_all):
        return jax.vmap(lambda a, b, c, e: slot_plan(a, b, c, e, EXPERTS, CAP))(
            ids_all.reshape(blocks, TOK_DEV, TOPK), keep_all.reshape(blocks, TOK_DEV, TOPK),
            slot_all.reshape(blocks, TOK_DEV, TOPK), level_all.reshape(blocks, TOK_DEV, TOPK))

    token_f, weight_f, live_f = plan_all(ids_fwd, keep_fwd, slot_fwd, level_fwd)
    token_b, weight_b, live_b = plan_all(ids_bwd, keep_bwd, slot_bwd, level_bwd)

    def pick(values, tokens_at, live_at):
        return jnp.where(live_at[:, None] > 0, values[tokens_at], jnp.zeros((), values.dtype))

    def scaled(values, tokens_at, weight_at):
        return (weight_at[:, None] * values[tokens_at].astype(jnp.float32)).astype(jnp.bfloat16)

    rows_in = jax.vmap(pick)(section_in.reshape(blocks, TOK_DEV, D), token_f, live_f)
    rows_saved = jax.vmap(pick)(section_saved.reshape(blocks, TOK_DEV, D), token_b, live_b)
    rows_cot = jax.vmap(scaled)(section_cot.reshape(blocks, TOK_DEV, D), token_b, weight_b)

    def to_expert(rows):
        return rows.reshape(blocks, EXPERTS, CAP, D).transpose(1, 0, 2, 3).reshape(EXPERTS, blocks * CAP, D)

    def from_expert(rows):
        return rows.reshape(EXPERTS, blocks, CAP, D).transpose(1, 0, 2, 3).reshape(blocks, EXPERTS * CAP, D)

    gate_full = gate_section.reshape(EXPERTS, 2, D, half_width).transpose(0, 2, 1, 3).reshape(EXPERTS, D, FE)
    up_full = up_section.reshape(EXPERTS, 2, D, half_width).transpose(0, 2, 1, 3).reshape(EXPERTS, D, FE)
    down_full = down_section.reshape(EXPERTS, FE, D)
    expert_out, expert_grad = lax.map(expert_pass, (to_expert(rows_in), to_expert(rows_saved), to_expert(rows_cot), gate_full, up_full, down_full))

    def combine(tokens_at, weight_at, rows):
        return jnp.zeros((TOK_DEV, D), jnp.float32).at[tokens_at].add(weight_at[:, None] * rows)

    routed_out = jax.vmap(combine)(token_f, weight_f, from_expert(expert_out)).reshape(TOKENS, D)
    routed_grad = jax.vmap(combine)(token_b, live_b, from_expert(expert_grad)).reshape(TOKENS, D)
    shared_out, shared_grad = shared_pass(section_in, section_saved, section_cot, shared_gate, shared_up, shared_down)
    return (shared_out + routed_out).astype(jnp.bfloat16), (shared_grad + routed_grad).astype(jnp.bfloat16)


def reference(inputs_prev, cotangent_next, saved_input, expert_ids, keep_mask, slot_pos, weight_q, gate_routed, up_routed, down_routed, gate_shared, up_shared, down_shared):
    forward_in = jnp.roll(inputs_prev, 1, axis=0)
    backward_in = jnp.roll(cotangent_next, -1, axis=0)
    out_act, in_grad = lax.map(one_section, (forward_in, saved_input, backward_in,
                                           expert_ids[0], keep_mask[0], slot_pos[0], weight_q[0],
                                           expert_ids[1], keep_mask[1], slot_pos[1], weight_q[1],
                                           gate_routed, up_routed, down_routed, gate_shared, up_shared, down_shared))
    return out_act, in_grad
```

```python
import jax
import jax.numpy as jnp
from jax import lax
from jax.sharding import PartitionSpec as P


def passed_along(block, axis, distance):
    devices = range(lax.axis_size(axis))
    route = [((i - distance) % len(devices), i) for i in devices]
    return lax.ppermute(block, axis, route)


def swish(values):
    return values * jax.nn.sigmoid(values)


def swish_slope(values):
    logistic = jax.nn.sigmoid(values)
    return logistic * (1.0 + values * (1.0 - logistic))


def contract_last(left, right):
    return lax.dot_general(
        left, right, (((1,), (1,)), ((), ())), preferred_element_type=jnp.float32
    )


def slot_plan(choice_ids, kept_flags, slot_index, weight_levels, total_slots, capacity):
    target = jnp.where(kept_flags > 0, choice_ids * capacity + slot_index, -1)
    slots = jnp.arange(total_slots, dtype=jnp.int32)
    match = target[None] == slots[:, None, None]
    chosen = jnp.sum(match.astype(jnp.int32), axis=2)
    level = jnp.sum(jnp.where(match, weight_levels[None], 0), axis=2)
    return chosen.astype(jnp.bfloat16), level


def section_link(values, offset):
    return passed_along(values, "pipe", offset)


def select_rows(chosen, values):
    return jnp.dot(chosen, values, preferred_element_type=jnp.float32)


def split_level(level):
    high = (level // 64).astype(jnp.float32) / 64.0
    low = (level % 64).astype(jnp.float32) / 4096.0
    return high.astype(jnp.bfloat16), low.astype(jnp.bfloat16)


def combine(factors, rows):
    return lax.dot_general(
        factors, rows, (((0,), (0,)), ((), ())), preferred_element_type=jnp.float32
    )


def other_sums(total, n_tensor):
    width = total.shape[1] // n_tensor
    me = lax.axis_index("tensor")
    mine = lax.dynamic_slice_in_dim(total, me * width, width, axis=1)
    for step in range(1, n_tensor):
        to = (me + step) % n_tensor
        piece = lax.dynamic_slice_in_dim(total, to * width, width, axis=1)
        mine = mine + passed_along(piece, "tensor", step)
    return mine


def expert_local(rows_in, rows_saved, rows_cot, gate_w, up_w, down_w):
    gate_pre = jnp.dot(rows_in, gate_w, preferred_element_type=jnp.float32)
    up_pre = jnp.dot(rows_in, up_w, preferred_element_type=jnp.float32)
    hidden = (swish(gate_pre) * up_pre).astype(jnp.bfloat16)
    result = jnp.dot(hidden, down_w, preferred_element_type=jnp.float32).astype(jnp.bfloat16)
    gate_back = jnp.dot(rows_saved, gate_w, preferred_element_type=jnp.float32)
    up_back = jnp.dot(rows_saved, up_w, preferred_element_type=jnp.float32)
    grad_hidden = contract_last(rows_cot, down_w)
    grad_gate = (grad_hidden * up_back * swish_slope(gate_back)).astype(jnp.bfloat16)
    grad_up = (grad_hidden * swish(gate_back)).astype(jnp.bfloat16)
    grad_rows = (contract_last(grad_gate, gate_w) + contract_last(grad_up, up_w)).astype(
        jnp.bfloat16
    )
    return (result, grad_rows)


def shared_pass(full_in, full_saved, full_cot, gate_w, up_w, down_w):
    gate_pre = jnp.dot(full_in, gate_w, preferred_element_type=jnp.float32)
    up_pre = jnp.dot(full_in, up_w, preferred_element_type=jnp.float32)
    hidden = (swish(gate_pre) * up_pre).astype(jnp.bfloat16)
    shared_out = jnp.dot(hidden, down_w, preferred_element_type=jnp.float32)
    gate_back = jnp.dot(full_saved, gate_w, preferred_element_type=jnp.float32)
    up_back = jnp.dot(full_saved, up_w, preferred_element_type=jnp.float32)
    grad_hidden = contract_last(full_cot, down_w)
    grad_gate = (grad_hidden * up_back * swish_slope(gate_back)).astype(jnp.bfloat16)
    grad_up = (grad_hidden * swish(gate_back)).astype(jnp.bfloat16)
    shared_grad = contract_last(grad_gate, gate_w) + contract_last(grad_up, up_w)
    return (shared_out, shared_grad)


def local(
    inputs_prev,
    cotangent_next,
    saved_input,
    expert_ids,
    keep_mask,
    slot_pos,
    weight_q,
    gate_routed,
    up_routed,
    down_routed,
    gate_shared,
    up_shared,
    down_shared,
):
    capacity = inputs_prev.shape[1] // 32
    n_expert = lax.axis_size("expert")
    n_tensor = lax.axis_size("tensor")
    experts_here = n_expert // 2
    slots = experts_here * capacity
    forward_in = section_link(inputs_prev[0], 1)
    backward_in = section_link(cotangent_next[0], -1)
    chosen_f, level_f = slot_plan(
        expert_ids[0, 0], keep_mask[0, 0], slot_pos[0, 0], weight_q[0, 0], slots, capacity
    )
    chosen_b, level_b = slot_plan(
        expert_ids[1, 0], keep_mask[1, 0], slot_pos[1, 0], weight_q[1, 0], slots, capacity
    )
    gate_w = gate_routed[0, 0]
    up_w = up_routed[0, 0]
    down_w = down_routed[0, 0]
    full_saved = lax.all_gather(saved_input[0], "tensor", axis=1, tiled=True)
    full_in = lax.all_gather(forward_in, "tensor", axis=1, tiled=True)
    full_cot = lax.all_gather(backward_in, "tensor", axis=1, tiled=True)
    feature_count = full_in.shape[1]
    weight_b = jnp.sum(level_b, axis=1).astype(jnp.float32) / 4096.0
    parcel = jnp.stack(
        (
            select_rows(chosen_f, full_in).astype(jnp.bfloat16),
            select_rows(chosen_b, full_saved).astype(jnp.bfloat16),
            (weight_b[:, None] * select_rows(chosen_b, full_cot)).astype(jnp.bfloat16),
        )
    ).reshape(3, experts_here, 1, capacity, feature_count)
    parcel = jnp.broadcast_to(parcel, (3, experts_here, 2, capacity, feature_count))
    parcel = parcel.reshape(3, n_expert, capacity, feature_count)
    pieces = lax.all_to_all(parcel, "expert", split_axis=1, concat_axis=1, tiled=True)
    rows = pieces.reshape(3, n_expert * capacity, feature_count)
    result, grad_rows = expert_local(rows[0], rows[1], rows[2], gate_w, up_w, down_w)
    returned = lax.all_to_all(
        jnp.stack((result, grad_rows)).reshape(2, n_expert, capacity, feature_count),
        "expert", split_axis=1, concat_axis=1, tiled=True,
    )
    back = returned.reshape(2, n_expert * capacity, feature_count)

    def doubled(factors):
        spread = factors.reshape(experts_here, 1, capacity, -1)
        spread = jnp.broadcast_to(spread, (experts_here, 2) + spread.shape[2:])
        return spread.reshape(n_expert * capacity, -1)

    high_f, low_f = split_level(level_f)
    factors_f = jnp.concatenate((doubled(high_f), doubled(low_f)), axis=0)
    routed_out = combine(factors_f, jnp.concatenate((back[0], back[0]), axis=0))
    routed_grad = combine(doubled(chosen_b), back[1])
    shared_out, shared_grad = shared_pass(
        full_in, full_saved, full_cot, gate_shared[0], up_shared[0], down_shared[0]
    )
    summed_out = other_sums(routed_out + shared_out, n_tensor)
    summed_grad = other_sums(routed_grad + shared_grad, n_tensor)
    return (summed_out.astype(jnp.bfloat16)[None], summed_grad.astype(jnp.bfloat16)[None])


def solution(mesh):
    return jax.shard_map(
        local,
        mesh=mesh,
        in_specs=(
            P("pipe", "expert", "tensor"),
            P("pipe", "expert", "tensor"),
            P("pipe", "expert", "tensor"),
            P(None, "pipe", "expert", None),
            P(None, "pipe", "expert", None),
            P(None, "pipe", "expert", None),
            P(None, "pipe", "expert", None),
            P("pipe", "expert", None, "tensor"),
            P("pipe", "expert", None, "tensor"),
            P("pipe", "expert", "tensor", None),
            P("pipe", None, "tensor"),
            P("pipe", None, "tensor"),
            P("pipe", "tensor", None),
        ),
        out_specs=(P("pipe", "expert", "tensor"), P("pipe", "expert", "tensor")),
        check_vma=False,
    )
```

```python
import functools

import jax
import jax.numpy as jnp
from jax import lax
from jax.experimental import pallas as pl
from jax.experimental.pallas import tpu as pltpu
from jax.sharding import PartitionSpec as P

MESH = pl.DeviceIdType.MESH
ROW_CHUNKS = 4
F32 = jnp.float32
BF16 = jnp.bfloat16


def swish(values):
    return values * jax.nn.sigmoid(values)


def swish_slope(values):
    logistic = jax.nn.sigmoid(values)
    return logistic * (1.0 + values * (1.0 - logistic))


def dot(left, right):
    return jnp.dot(left, right, preferred_element_type=F32)


def contract_last(left, right):
    return lax.dot_general(left, right, (((1,), (1,)), ((), ())), preferred_element_type=F32)


def chunk_of(width):
    return 256 if width % 256 == 0 else 128


def kernel(
    sizes,
    x_prev, c_next, saved, ids, keep, slot, level,
    gate_r_hbm, up_r_hbm, down_r_hbm, gate_s_hbm, up_s_hbm, down_s_hbm,
    out_ref, grad_ref,
    gate_r, up_r, down_r, gate_s, up_s, down_s,
    full_x, full_c, full_s,
    a_saved, b_saved, hidden, grad_gate, grad_up,
    a_routed, b_routed,
    send_early, send_late, recv_early, recv_late, rows_early, rows_late,
    ret_send, ret_recv, ret_rows,
    part_out, part_grad, peer_out, peer_grad,
    weight_sem, saved_sem, saved_send, saved_recv,
    pipe_send, pipe_recv, fwd_send, fwd_recv,
    early_send, early_recv, late_send, late_recv, self_sem,
    ret_ssem, ret_rsem, part_send, part_recv,
):
    n_pipe, ne, nt, capacity = sizes
    tokens, width = x_prev.shape
    features = width * nt
    experts = ne // 2
    group = 2 * capacity
    me_p, me_e, me_t = lax.axis_index("pipe"), lax.axis_index("expert"), lax.axis_index("tensor")
    nxt, prv = lax.rem(me_p + 1, n_pipe), lax.rem(me_p + n_pipe - 1, n_pipe)
    my_cols = pl.ds(pl.multiple_of(me_t * width, 128), width)

    def peer_t(step):
        return lax.rem(me_t + step, nt)

    def peer_e(step):
        return lax.rem(me_e + step, ne)

    def remote(src, dst, ssem, rsem, device):
        return pltpu.make_async_remote_copy(
            src_ref=src, dst_ref=dst, send_sem=ssem, recv_sem=rsem,
            device_id=device, device_id_type=MESH,
        )

    saved_local = pltpu.make_async_copy(saved, full_s.at[:, my_cols], saved_sem)
    saved_local.start()
    loads = {}
    pairs = (
        (gate_s_hbm, gate_s), (up_s_hbm, up_s), (gate_r_hbm, gate_r),
        (up_r_hbm, up_r), (down_s_hbm, down_s), (down_r_hbm, down_r),
    )
    for n, (src, dst) in enumerate(pairs):
        loads[n] = pltpu.make_async_copy(src, dst, weight_sem.at[n])
        loads[n].start()

    barrier = pltpu.get_barrier_semaphore()
    greeted = [{"pipe": nxt}, {"pipe": prv}]
    for se in range(ne):
        for st in range(nt):
            if se or st:
                greeted.append({"expert": peer_e(se), "tensor": peer_t(st)})
    for device in greeted:
        pl.semaphore_signal(barrier, inc=1, device_id=device, device_id_type=MESH)
    pl.semaphore_wait(barrier, len(greeted))

    step_rows = tokens // ROW_CHUNKS
    pipe_copies = []
    for q in range(ROW_CHUNKS):
        rows = pl.ds(q * step_rows, step_rows)
        for a, (src, dst, to) in enumerate(((x_prev, full_x, nxt), (c_next, full_c, prv))):
            copy = remote(
                src.at[rows, :], dst.at[rows, my_cols],
                pipe_send.at[a, q], pipe_recv.at[a, q], {"pipe": to},
            )
            copy.start()
            pipe_copies.append(copy)
    saved_copies = []
    for st in range(1, nt):
        copy = remote(
            saved, full_s.at[:, my_cols], saved_send.at[st - 1], saved_recv.at[st - 1],
            {"tensor": peer_t(st)},
        )
        copy.start()
        saved_copies.append(copy)

    def targets(m):
        return jnp.where(keep[m] > 0, ids[m] * capacity + slot[m], -1)

    target_f, target_b = targets(0), targets(1)

    def table(target, values, slots_at):
        total = jnp.zeros((tokens, slots_at.shape[1]), jnp.int32)
        for k in range(target.shape[1]):
            total = total + jnp.where(target[:, k:k + 1] == slots_at, values[:, k:k + 1], 0)
        return total

    lanes = ((experts * group + 127) // 128) * 128
    place = lax.broadcasted_iota(jnp.int32, (tokens, lanes), 1)
    inside = lax.rem(place, group)
    owner = lax.div(place, group)
    slots_x = jnp.where(inside < capacity, owner * capacity + inside, -2)
    slots_c = jnp.where(inside >= capacity, owner * capacity + inside - capacity, -2)
    ones = jnp.ones(target_f.shape, jnp.int32)
    used = experts * group
    pick_x = table(target_f, ones, slots_x).astype(F32).T[:used].astype(BF16)
    pick_c = table(target_b, ones, slots_c).astype(F32).T[:used].astype(BF16)
    scale_c = jnp.sum(
        table(target_b, level[1], slots_c).astype(F32).T[:used], axis=1, keepdims=True
    ) / 4096.0

    parts = ne * nt * group
    lanes = ((parts + 127) // 128) * 128
    place = lax.broadcasted_iota(jnp.int32, (tokens, lanes), 1)
    inside = lax.rem(place, group)
    owner = lax.div(place, 2 * nt * group)
    slots_o = jnp.where(inside < capacity, owner * capacity + inside, -2)
    slots_g = jnp.where(inside >= capacity, owner * capacity + inside - capacity, -2)
    level_o = table(target_f, level[0], slots_o)
    high = lax.div(level_o, 64)
    low = level_o - high * 64
    factor_high = (high.astype(F32) / 64.0).astype(BF16)[:, :parts]
    factor_low = (low.astype(F32) / 4096.0).astype(BF16)[:, :parts]
    factor_grad = table(target_b, ones, slots_g).astype(F32).astype(BF16)[:, :parts]

    saved_local.wait()
    for copy in saved_copies:
        copy.wait_recv()
    cf = chunk_of(features)

    def exchange(buffer, landing, ssem, rsem, self_index):
        copies = []
        for se in range(1, ne):
            to = peer_e(se)
            copy = remote(
                buffer.at[lax.div(to, 2)], landing.at[me_e], ssem.at[se - 1], rsem.at[se - 1],
                {"expert": to},
            )
            copy.start()
            copies.append(copy)
        own = pltpu.make_async_copy(
            buffer.at[lax.div(me_e, 2)], landing.at[me_e], self_sem.at[self_index]
        )
        own.start()
        return copies, own

    def early_rows(n, carry):
        cols = pl.ds(pl.multiple_of(n * cf, 128), cf)
        picked = dot(pick_c, full_s[:, cols])
        for e in range(experts):
            send_early[e, :, cols] = picked[e * group:(e + 1) * group].astype(BF16)
        return carry

    lax.fori_loop(0, features // cf, early_rows, 0)
    early_copies, early_own = exchange(send_early, recv_early, early_send, early_recv, 0)

    def gather_rows(landing, dest):
        for i in range(0, ne, 2):
            both = jnp.concatenate(
                (landing[i].astype(F32), landing[i + 1].astype(F32)), axis=0
            )
            dest[i * group:(i + 2) * group, :] = both.astype(BF16)

    loads[0].wait()
    loads[1].wait()
    cs = chunk_of(gate_s.shape[1])

    def shared_saved(n, carry):
        cols = pl.ds(pl.multiple_of(n * cs, 128), cs)
        a_saved[:, cols] = dot(full_s[...], gate_s[:, cols])
        b_saved[:, cols] = dot(full_s[...], up_s[:, cols])
        return carry

    lax.fori_loop(0, gate_s.shape[1] // cs, shared_saved, 0)

    fwd_copies = []

    def forward(q):
        rows = pl.ds(q * step_rows, step_rows)
        for a, held in enumerate((full_x, full_c)):
            pipe_copies[2 * q + a].wait_recv()
            for st in range(1, nt):
                copy = remote(
                    held.at[rows, my_cols], held.at[rows, my_cols],
                    fwd_send.at[a, q, st - 1], fwd_recv.at[a, q, st - 1], {"tensor": peer_t(st)},
                )
                copy.start()
                fwd_copies.append(copy)

    for q in range(ROW_CHUNKS // 2):
        forward(q)

    for copy in early_copies:
        copy.wait_recv()
    early_own.wait()
    gather_rows(recv_early, rows_early)
    loads[2].wait()
    loads[3].wait()
    a_routed[...] = dot(rows_early[...], gate_r[...])
    b_routed[...] = dot(rows_early[...], up_r[...])

    for q in range(ROW_CHUNKS // 2, ROW_CHUNKS):
        forward(q)
    for copy in fwd_copies:
        copy.wait_recv()

    def late_rows(n, carry):
        cols = pl.ds(pl.multiple_of(n * cf, 128), cf)
        picked = dot(pick_x, full_x[:, cols]) + scale_c * dot(pick_c, full_c[:, cols])
        for e in range(experts):
            send_late[e, :, cols] = picked[e * group:(e + 1) * group].astype(BF16)
        return carry

    lax.fori_loop(0, features // cf, late_rows, 0)
    late_copies, late_own = exchange(send_late, recv_late, late_send, late_recv, 1)

    loads[4].wait()

    def shared_first(n, carry):
        cols = pl.ds(pl.multiple_of(n * cs, 128), cs)
        gate_pre = dot(full_x[...], gate_s[:, cols])
        up_pre = dot(full_x[...], up_s[:, cols])
        hidden[:, cols] = (swish(gate_pre) * up_pre).astype(BF16)
        grad_hidden = contract_last(full_c[...], down_s[cols, :])
        gate_back = a_saved[:, cols]
        grad_gate[:, cols] = (grad_hidden * b_saved[:, cols] * swish_slope(gate_back)).astype(BF16)
        grad_up[:, cols] = (grad_hidden * swish(gate_back)).astype(BF16)
        return carry

    lax.fori_loop(0, gate_s.shape[1] // cs, shared_first, 0)

    loads[5].wait()
    for copy in late_copies:
        copy.wait_recv()
    late_own.wait()
    gather_rows(recv_late, rows_late)
    gate_pre = dot(rows_late[...], gate_r[...])
    up_pre = dot(rows_late[...], up_r[...])
    grad_hidden = contract_last(rows_late[...], down_r[...])
    gate_back = a_routed[...]
    row = lax.broadcasted_iota(jnp.int32, gate_pre.shape, 0)
    ahead = lax.rem(row, group) < capacity
    hidden_r = jnp.where(ahead, swish(gate_pre) * up_pre, 0.0).astype(BF16)
    gate_grad_r = jnp.where(
        ahead, 0.0, grad_hidden * b_routed[...] * swish_slope(gate_back)
    ).astype(BF16)
    up_grad_r = jnp.where(ahead, 0.0, grad_hidden * swish(gate_back)).astype(BF16)
    cw = chunk_of(width)
    for c in range(nt):
        def routed_second(n, carry, c=c):
            at = pl.ds(pl.multiple_of(n * cw, 128), cw)
            cols = pl.ds(pl.multiple_of(c * width + n * cw, 128), cw)
            total = (
                dot(hidden_r, down_r[:, cols])
                + contract_last(gate_grad_r, gate_r[cols, :])
                + contract_last(up_grad_r, up_r[cols, :])
            )
            for i in range(ne):
                ret_send[i, c, :, at] = total[i * group:(i + 1) * group].astype(BF16)
            return carry

        lax.fori_loop(0, width // cw, routed_second, 0)

    ret_copies = []
    for se in range(ne):
        for st in range(nt):
            if se or st:
                to_e, to_t = peer_e(se), peer_t(st)
                n = se * nt + st - 1
                copy = remote(
                    ret_send.at[to_e, to_t], ret_recv.at[me_e, me_t],
                    ret_ssem.at[n], ret_rsem.at[n], {"expert": to_e, "tensor": to_t},
                )
                copy.start()
                ret_copies.append(copy)
    ret_own = pltpu.make_async_copy(
        ret_send.at[me_e, me_t], ret_recv.at[me_e, me_t], self_sem.at[2]
    )
    ret_own.start()

    part_copies = []
    for st in list(range(1, nt)) + [0]:
        to = peer_t(st)

        def shared_second(n, carry, st=st, to=to):
            at = pl.ds(pl.multiple_of(n * cw, 128), cw)
            cols = pl.ds(pl.multiple_of(to * width + n * cw, 128), cw)
            part_out[st, :, at] = dot(hidden[...], down_s[:, cols])
            part_grad[st, :, at] = contract_last(grad_gate[...], gate_s[cols, :]) + contract_last(
                grad_up[...], up_s[cols, :]
            )
            return carry

        lax.fori_loop(0, width // cw, shared_second, 0)
        if st:
            for a, (src, dst) in enumerate(((part_out, peer_out), (part_grad, peer_grad))):
                copy = remote(
                    src.at[st], dst.at[st - 1], part_send.at[a, st - 1], part_recv.at[a, st - 1],
                    {"tensor": to},
                )
                copy.start()
                part_copies.append(copy)

    for copy in ret_copies:
        copy.wait_recv()
    ret_own.wait()
    for i in range(0, ne * nt, 2):
        first, second = divmod(i, nt), divmod(i + 1, nt)
        both = jnp.concatenate((ret_recv[first].astype(F32), ret_recv[second].astype(F32)), axis=0)
        ret_rows[i * group:(i + 2) * group, :] = both.astype(BF16)
    for copy in part_copies:
        copy.wait_recv()

    def finish(n, carry):
        at = pl.ds(pl.multiple_of(n * cw, 128), cw)
        rows = ret_rows[:, at]
        out_sum = part_out[0, :, at] + (dot(factor_high, rows) + dot(factor_low, rows))
        grad_sum = part_grad[0, :, at] + dot(factor_grad, rows)
        for st in range(1, nt):
            out_sum = out_sum + peer_out[st - 1, :, at]
            grad_sum = grad_sum + peer_grad[st - 1, :, at]
        out_ref[:, at] = out_sum.astype(BF16)
        grad_ref[:, at] = grad_sum.astype(BF16)
        return carry

    lax.fori_loop(0, width // cw, finish, 0)

    for copy in (
        pipe_copies + saved_copies + fwd_copies + early_copies + late_copies + ret_copies
        + part_copies
    ):
        copy.wait_send()


def local(
    inputs_prev, cotangent_next, saved_input, expert_ids, keep_mask, slot_pos, weight_q,
    gate_routed, up_routed, down_routed, gate_shared, up_shared, down_shared,
):
    n_pipe, ne, nt = lax.axis_size("pipe"), lax.axis_size("expert"), lax.axis_size("tensor")
    tokens, width = inputs_prev.shape[1:]
    features = width * nt
    capacity = tokens // 32
    group = 2 * capacity
    experts = ne // 2
    fr, fs = gate_routed.shape[3], gate_shared.shape[2]
    vmem = pl.BlockSpec(memory_space=pltpu.VMEM)
    hbm = pl.BlockSpec(memory_space=pl.ANY)
    dma = pltpu.SemaphoreType.DMA
    shape = jax.ShapeDtypeStruct((tokens, width), BF16)
    out, grad = pl.pallas_call(
        functools.partial(kernel, (n_pipe, ne, nt, capacity)),
        out_shape=(shape, shape),
        in_specs=[hbm] * 3 + [vmem] * 4 + [hbm] * 6,
        out_specs=(vmem, vmem),
        scratch_shapes=[
            pltpu.VMEM((features, fr), BF16),
            pltpu.VMEM((features, fr), BF16),
            pltpu.VMEM((fr, features), BF16),
            pltpu.VMEM((features, fs), BF16),
            pltpu.VMEM((features, fs), BF16),
            pltpu.VMEM((fs, features), BF16),
            pltpu.VMEM((tokens, features), BF16),
            pltpu.VMEM((tokens, features), BF16),
            pltpu.VMEM((tokens, features), BF16),
            pltpu.VMEM((tokens, fs), F32),
            pltpu.VMEM((tokens, fs), F32),
            pltpu.VMEM((tokens, fs), BF16),
            pltpu.VMEM((tokens, fs), BF16),
            pltpu.VMEM((tokens, fs), BF16),
            pltpu.VMEM((ne * group, fr), F32),
            pltpu.VMEM((ne * group, fr), F32),
            pltpu.VMEM((experts, group, features), BF16),
            pltpu.VMEM((experts, group, features), BF16),
            pltpu.VMEM((ne, group, features), BF16),
            pltpu.VMEM((ne, group, features), BF16),
            pltpu.VMEM((ne * group, features), BF16),
            pltpu.VMEM((ne * group, features), BF16),
            pltpu.VMEM((ne, nt, group, width), BF16),
            pltpu.VMEM((ne, nt, group, width), BF16),
            pltpu.VMEM((ne * nt * group, width), BF16),
            pltpu.VMEM((nt, tokens, width), F32),
            pltpu.VMEM((nt, tokens, width), F32),
            pltpu.VMEM((nt - 1, tokens, width), F32),
            pltpu.VMEM((nt - 1, tokens, width), F32),
            dma((6,)),
            dma,
            dma((nt - 1,)),
            dma((nt - 1,)),
            dma((2, ROW_CHUNKS)),
            dma((2, ROW_CHUNKS)),
            dma((2, ROW_CHUNKS, nt - 1)),
            dma((2, ROW_CHUNKS, nt - 1)),
            dma((ne - 1,)),
            dma((ne - 1,)),
            dma((ne - 1,)),
            dma((ne - 1,)),
            dma((3,)),
            dma((ne * nt - 1,)),
            dma((ne * nt - 1,)),
            dma((2, nt - 1)),
            dma((2, nt - 1)),
        ],
        compiler_params=pltpu.CompilerParams(collective_id=0, has_side_effects=True),
        name="moe_step",
    )(
        inputs_prev[0], cotangent_next[0], saved_input[0],
        expert_ids[:, 0], keep_mask[:, 0], slot_pos[:, 0], weight_q[:, 0],
        gate_routed[0, 0], up_routed[0, 0], down_routed[0, 0],
        gate_shared[0], up_shared[0], down_shared[0],
    )
    return out[None], grad[None]


def solution(mesh):
    return jax.shard_map(
        local,
        mesh=mesh,
        in_specs=(
            P("pipe", "expert", "tensor"),
            P("pipe", "expert", "tensor"),
            P("pipe", "expert", "tensor"),
            P(None, "pipe", "expert", None),
            P(None, "pipe", "expert", None),
            P(None, "pipe", "expert", None),
            P(None, "pipe", "expert", None),
            P("pipe", "expert", None, "tensor"),
            P("pipe", "expert", None, "tensor"),
            P("pipe", "expert", "tensor", None),
            P("pipe", None, "tensor"),
            P("pipe", None, "tensor"),
            P("pipe", "tensor", None),
        ),
        out_specs=(P("pipe", "expert", "tensor"), P("pipe", "expert", "tensor")),
        check_vma=False,
    )
```

```python
import functools

import jax
import jax.numpy as jnp
from jax import lax
from jax.experimental import pallas as pl
from jax.experimental.pallas import tpu as pltpu
from jax.sharding import PartitionSpec as P

MESH = pl.DeviceIdType.MESH
ROW_CHUNKS = 4
F32 = jnp.float32
BF16 = jnp.bfloat16


def swish(values):
    return values * jax.nn.sigmoid(values)


def swish_slope(values):
    logistic = jax.nn.sigmoid(values)
    return logistic * (1.0 + values * (1.0 - logistic))


def dot(left, right):
    return jnp.dot(left, right, preferred_element_type=F32)


def contract_last(left, right):
    return lax.dot_general(left, right, (((1,), (1,)), ((), ())), preferred_element_type=F32)


def chunk_of(width):
    return 256 if width % 256 == 0 else 128


def kernel(
    sizes,
    x_prev, c_next, saved, ids, keep, slot, level,
    gate_r_hbm, up_r_hbm, down_r_hbm, gate_s_hbm, up_s_hbm, down_s_hbm,
    out_ref, grad_ref,
    gate_r, up_r, down_r, gate_s, up_s, down_s,
    full_x, full_c, full_s,
    a_saved, b_saved, hidden, grad_gate, grad_up,
    a_routed, b_routed,
    send_early, send_late, recv_early, recv_late, rows_early, rows_late,
    ret_send, ret_recv, ret_rows,
    part_out, part_grad, peer_out, peer_grad,
    weight_sem, saved_sem, saved_send, saved_recv,
    pipe_send, pipe_recv, fwd_send, fwd_recv,
    early_send, early_recv, late_send, late_recv, self_sem,
    ret_ssem, ret_rsem, part_send, part_recv,
):
    n_pipe, ne, nt, capacity = sizes
    tokens, width = x_prev.shape
    features = width * nt
    experts = ne // 2
    group = 2 * capacity
    me_p, me_e, me_t = lax.axis_index("pipe"), lax.axis_index("expert"), lax.axis_index("tensor")
    nxt, prv = lax.rem(me_p + 1, n_pipe), lax.rem(me_p + n_pipe - 1, n_pipe)
    my_cols = pl.ds(pl.multiple_of(me_t * width, 128), width)

    def peer_t(step):
        return lax.rem(me_t + step, nt)

    def peer_e(step):
        return lax.rem(me_e + step, ne)

    def remote(src, dst, ssem, rsem, device):
        return pltpu.make_async_remote_copy(
            src_ref=src, dst_ref=dst, send_sem=ssem, recv_sem=rsem,
            device_id=device, device_id_type=MESH,
        )

    saved_local = pltpu.make_async_copy(saved, full_s.at[:, my_cols], saved_sem)
    saved_local.start()
    loads = {}
    pairs = (
        (gate_s_hbm, gate_s), (up_s_hbm, up_s), (gate_r_hbm, gate_r),
        (up_r_hbm, up_r), (down_s_hbm, down_s), (down_r_hbm, down_r),
    )
    for n, (src, dst) in enumerate(pairs):
        loads[n] = pltpu.make_async_copy(src, dst, weight_sem.at[n])
        loads[n].start()

    barrier = pltpu.get_barrier_semaphore()
    greeted = [{"pipe": nxt}, {"pipe": prv}]
    for se in range(ne):
        for st in range(nt):
            if se or st:
                greeted.append({"expert": peer_e(se), "tensor": peer_t(st)})
    for device in greeted:
        pl.semaphore_signal(barrier, inc=1, device_id=device, device_id_type=MESH)
    pl.semaphore_wait(barrier, len(greeted))

    step_rows = tokens // ROW_CHUNKS
    pipe_copies = []
    for q in range(ROW_CHUNKS):
        rows = pl.ds(q * step_rows, step_rows)
        for a, (src, dst, to) in enumerate(((x_prev, full_x, nxt), (c_next, full_c, prv))):
            copy = remote(
                src.at[rows, :], dst.at[rows, my_cols],
                pipe_send.at[a, q], pipe_recv.at[a, q], {"pipe": to},
            )
            copy.start()
            pipe_copies.append(copy)
    saved_copies = []
    for st in range(1, nt):
        copy = remote(
            saved, full_s.at[:, my_cols], saved_send.at[st - 1], saved_recv.at[st - 1],
            {"tensor": peer_t(st)},
        )
        copy.start()
        saved_copies.append(copy)

    def targets(m):
        return jnp.where(keep[m] > 0, ids[m] * capacity + slot[m], -1)

    target_f, target_b = targets(0), targets(1)

    def table(target, values, slots_at):
        total = jnp.zeros((slots_at.shape[0], tokens), jnp.int32)
        for k in range(target.shape[0]):
            total = total + jnp.where(target[k:k + 1] == slots_at, values[k:k + 1], 0)
        return total

    used = experts * group
    place = lax.broadcasted_iota(jnp.int32, (used, tokens), 0)
    inside = lax.rem(place, group)
    owner = lax.div(place, group)
    slots_x = jnp.where(inside < capacity, owner * capacity + inside, -2)
    slots_c = jnp.where(inside >= capacity, owner * capacity + inside - capacity, -2)
    ones = jnp.ones(target_f.shape, jnp.int32)
    pick_x = table(target_f, ones, slots_x).astype(F32).astype(BF16)
    pick_c = table(target_b, ones, slots_c).astype(F32).astype(BF16)
    scale_c = jnp.sum(
        table(target_b, level[1], slots_c).astype(F32), axis=1, keepdims=True
    ) / 4096.0

    parts = ne * nt * group
    place = lax.broadcasted_iota(jnp.int32, (parts, tokens), 0)
    inside = lax.rem(place, group)
    owner = lax.div(place, 2 * nt * group)
    slots_o = jnp.where(inside < capacity, owner * capacity + inside, -2)
    slots_g = jnp.where(inside >= capacity, owner * capacity + inside - capacity, -2)
    level_o = table(target_f, level[0], slots_o)
    high = lax.div(level_o, 64)
    low = level_o - high * 64
    factor_high = (high.astype(F32) / 64.0).T.astype(BF16)
    factor_low = (low.astype(F32) / 4096.0).T.astype(BF16)
    factor_grad = table(target_b, ones, slots_g).astype(F32).T.astype(BF16)

    saved_local.wait()
    for copy in saved_copies:
        copy.wait_recv()
    cf = chunk_of(features)

    def exchange(buffer, landing, ssem, rsem, self_index):
        copies = []
        for se in range(1, ne):
            to = peer_e(se)
            copy = remote(
                buffer.at[lax.div(to, 2)], landing.at[me_e], ssem.at[se - 1], rsem.at[se - 1],
                {"expert": to},
            )
            copy.start()
            copies.append(copy)
        own = pltpu.make_async_copy(
            buffer.at[lax.div(me_e, 2)], landing.at[me_e], self_sem.at[self_index]
        )
        own.start()
        return copies, own

    def early_rows(n, carry):
        cols = pl.ds(pl.multiple_of(n * cf, 128), cf)
        picked = dot(pick_c, full_s[:, cols])
        for e in range(experts):
            send_early[e, :, cols] = picked[e * group:(e + 1) * group].astype(BF16)
        return carry

    lax.fori_loop(0, features // cf, early_rows, 0)
    early_copies, early_own = exchange(send_early, recv_early, early_send, early_recv, 0)

    def gather_rows(landing, dest):
        for i in range(0, ne, 2):
            both = jnp.concatenate(
                (landing[i].astype(F32), landing[i + 1].astype(F32)), axis=0
            )
            dest[i * group:(i + 2) * group, :] = both.astype(BF16)

    loads[0].wait()
    loads[1].wait()
    cs = chunk_of(gate_s.shape[1])

    def shared_saved(n, carry):
        cols = pl.ds(pl.multiple_of(n * cs, 128), cs)
        a_saved[:, cols] = dot(full_s[...], gate_s[:, cols])
        b_saved[:, cols] = dot(full_s[...], up_s[:, cols])
        return carry

    lax.fori_loop(0, gate_s.shape[1] // cs, shared_saved, 0)

    fwd_copies = []

    def forward(q):
        rows = pl.ds(q * step_rows, step_rows)
        for a, held in enumerate((full_x, full_c)):
            pipe_copies[2 * q + a].wait_recv()
            for st in range(1, nt):
                copy = remote(
                    held.at[rows, my_cols], held.at[rows, my_cols],
                    fwd_send.at[a, q, st - 1], fwd_recv.at[a, q, st - 1], {"tensor": peer_t(st)},
                )
                copy.start()
                fwd_copies.append(copy)

    for q in range(ROW_CHUNKS // 2):
        forward(q)

    for copy in early_copies:
        copy.wait_recv()
    early_own.wait()
    gather_rows(recv_early, rows_early)
    loads[2].wait()
    loads[3].wait()
    a_routed[...] = dot(rows_early[...], gate_r[...])
    b_routed[...] = dot(rows_early[...], up_r[...])

    for q in range(ROW_CHUNKS // 2, ROW_CHUNKS):
        forward(q)
    for copy in fwd_copies:
        copy.wait_recv()

    def late_rows(n, carry):
        cols = pl.ds(pl.multiple_of(n * cf, 128), cf)
        picked = dot(pick_x, full_x[:, cols]) + scale_c * dot(pick_c, full_c[:, cols])
        for e in range(experts):
            send_late[e, :, cols] = picked[e * group:(e + 1) * group].astype(BF16)
        return carry

    lax.fori_loop(0, features // cf, late_rows, 0)
    late_copies, late_own = exchange(send_late, recv_late, late_send, late_recv, 1)

    loads[4].wait()

    def shared_first(n, carry):
        cols = pl.ds(pl.multiple_of(n * cs, 128), cs)
        gate_pre = dot(full_x[...], gate_s[:, cols])
        up_pre = dot(full_x[...], up_s[:, cols])
        hidden[:, cols] = (swish(gate_pre) * up_pre).astype(BF16)
        grad_hidden = contract_last(full_c[...], down_s[cols, :])
        gate_back = a_saved[:, cols]
        grad_gate[:, cols] = (grad_hidden * b_saved[:, cols] * swish_slope(gate_back)).astype(BF16)
        grad_up[:, cols] = (grad_hidden * swish(gate_back)).astype(BF16)
        return carry

    lax.fori_loop(0, gate_s.shape[1] // cs, shared_first, 0)

    loads[5].wait()
    for copy in late_copies:
        copy.wait_recv()
    late_own.wait()
    gather_rows(recv_late, rows_late)
    gate_pre = dot(rows_late[...], gate_r[...])
    up_pre = dot(rows_late[...], up_r[...])
    grad_hidden = contract_last(rows_late[...], down_r[...])
    gate_back = a_routed[...]
    row = lax.broadcasted_iota(jnp.int32, gate_pre.shape, 0)
    ahead = lax.rem(row, group) < capacity
    hidden_r = jnp.where(ahead, swish(gate_pre) * up_pre, 0.0).astype(BF16)
    gate_grad_r = jnp.where(
        ahead, 0.0, grad_hidden * b_routed[...] * swish_slope(gate_back)
    ).astype(BF16)
    up_grad_r = jnp.where(ahead, 0.0, grad_hidden * swish(gate_back)).astype(BF16)
    cw = chunk_of(width)
    ret_copies = []
    for st in list(range(1, nt)) + [0]:
        to_t = peer_t(st)

        def routed_second(n, carry, to_t=to_t):
            at = pl.ds(pl.multiple_of(n * cw, 128), cw)
            cols = pl.ds(pl.multiple_of(to_t * width + n * cw, 128), cw)
            total = (
                dot(hidden_r, down_r[:, cols])
                + contract_last(gate_grad_r, gate_r[cols, :])
                + contract_last(up_grad_r, up_r[cols, :])
            )
            for i in range(ne):
                ret_send[i, to_t, :, at] = total[i * group:(i + 1) * group].astype(BF16)
            return carry

        lax.fori_loop(0, width // cw, routed_second, 0)
        for se in range(ne):
            if se or st:
                to_e = peer_e(se)
                n = se * nt + st - 1
                copy = remote(
                    ret_send.at[to_e, to_t], ret_recv.at[me_e, me_t],
                    ret_ssem.at[n], ret_rsem.at[n], {"expert": to_e, "tensor": to_t},
                )
                copy.start()
                ret_copies.append(copy)
    ret_own = pltpu.make_async_copy(
        ret_send.at[me_e, me_t], ret_recv.at[me_e, me_t], self_sem.at[2]
    )
    ret_own.start()

    part_copies = []
    for st in list(range(1, nt)) + [0]:
        to = peer_t(st)

        def shared_second(n, carry, st=st, to=to):
            at = pl.ds(pl.multiple_of(n * cw, 128), cw)
            cols = pl.ds(pl.multiple_of(to * width + n * cw, 128), cw)
            part_out[st, :, at] = dot(hidden[...], down_s[:, cols])
            part_grad[st, :, at] = contract_last(grad_gate[...], gate_s[cols, :]) + contract_last(
                grad_up[...], up_s[cols, :]
            )
            return carry

        lax.fori_loop(0, width // cw, shared_second, 0)
        if st:
            for a, (src, dst) in enumerate(((part_out, peer_out), (part_grad, peer_grad))):
                copy = remote(
                    src.at[st], dst.at[st - 1], part_send.at[a, st - 1], part_recv.at[a, st - 1],
                    {"tensor": to},
                )
                copy.start()
                part_copies.append(copy)

    for copy in ret_copies:
        copy.wait_recv()
    ret_own.wait()
    for i in range(0, ne * nt, 2):
        first, second = divmod(i, nt), divmod(i + 1, nt)
        both = jnp.concatenate((ret_recv[first].astype(F32), ret_recv[second].astype(F32)), axis=0)
        ret_rows[i * group:(i + 2) * group, :] = both.astype(BF16)
    for copy in part_copies:
        copy.wait_recv()

    def finish(n, carry):
        at = pl.ds(pl.multiple_of(n * cw, 128), cw)
        rows = ret_rows[:, at]
        out_sum = part_out[0, :, at] + (dot(factor_high, rows) + dot(factor_low, rows))
        grad_sum = part_grad[0, :, at] + dot(factor_grad, rows)
        for st in range(1, nt):
            out_sum = out_sum + peer_out[st - 1, :, at]
            grad_sum = grad_sum + peer_grad[st - 1, :, at]
        out_ref[:, at] = out_sum.astype(BF16)
        grad_ref[:, at] = grad_sum.astype(BF16)
        return carry

    lax.fori_loop(0, width // cw, finish, 0)

    for copy in (
        pipe_copies + saved_copies + fwd_copies + early_copies + late_copies + ret_copies
        + part_copies
    ):
        copy.wait_send()


def lanes_last(choices):
    return jnp.swapaxes(choices[:, 0], 1, 2)


def local(
    inputs_prev, cotangent_next, saved_input, expert_ids, keep_mask, slot_pos, weight_q,
    gate_routed, up_routed, down_routed, gate_shared, up_shared, down_shared,
):
    n_pipe, ne, nt = lax.axis_size("pipe"), lax.axis_size("expert"), lax.axis_size("tensor")
    tokens, width = inputs_prev.shape[1:]
    features = width * nt
    capacity = tokens // 32
    group = 2 * capacity
    experts = ne // 2
    fr, fs = gate_routed.shape[3], gate_shared.shape[2]
    vmem = pl.BlockSpec(memory_space=pltpu.VMEM)
    hbm = pl.BlockSpec(memory_space=pl.ANY)
    dma = pltpu.SemaphoreType.DMA
    shape = jax.ShapeDtypeStruct((tokens, width), BF16)
    out, grad = pl.pallas_call(
        functools.partial(kernel, (n_pipe, ne, nt, capacity)),
        out_shape=(shape, shape),
        in_specs=[hbm] * 3 + [vmem] * 4 + [hbm] * 6,
        out_specs=(vmem, vmem),
        scratch_shapes=[
            pltpu.VMEM((features, fr), BF16),
            pltpu.VMEM((features, fr), BF16),
            pltpu.VMEM((fr, features), BF16),
            pltpu.VMEM((features, fs), BF16),
            pltpu.VMEM((features, fs), BF16),
            pltpu.VMEM((fs, features), BF16),
            pltpu.VMEM((tokens, features), BF16),
            pltpu.VMEM((tokens, features), BF16),
            pltpu.VMEM((tokens, features), BF16),
            pltpu.VMEM((tokens, fs), F32),
            pltpu.VMEM((tokens, fs), F32),
            pltpu.VMEM((tokens, fs), BF16),
            pltpu.VMEM((tokens, fs), BF16),
            pltpu.VMEM((tokens, fs), BF16),
            pltpu.VMEM((ne * group, fr), F32),
            pltpu.VMEM((ne * group, fr), F32),
            pltpu.VMEM((experts, group, features), BF16),
            pltpu.VMEM((experts, group, features), BF16),
            pltpu.VMEM((ne, group, features), BF16),
            pltpu.VMEM((ne, group, features), BF16),
            pltpu.VMEM((ne * group, features), BF16),
            pltpu.VMEM((ne * group, features), BF16),
            pltpu.VMEM((ne, nt, group, width), BF16),
            pltpu.VMEM((ne, nt, group, width), BF16),
            pltpu.VMEM((ne * nt * group, width), BF16),
            pltpu.VMEM((nt, tokens, width), F32),
            pltpu.VMEM((nt, tokens, width), F32),
            pltpu.VMEM((nt - 1, tokens, width), F32),
            pltpu.VMEM((nt - 1, tokens, width), F32),
            dma((6,)),
            dma,
            dma((nt - 1,)),
            dma((nt - 1,)),
            dma((2, ROW_CHUNKS)),
            dma((2, ROW_CHUNKS)),
            dma((2, ROW_CHUNKS, nt - 1)),
            dma((2, ROW_CHUNKS, nt - 1)),
            dma((ne - 1,)),
            dma((ne - 1,)),
            dma((ne - 1,)),
            dma((ne - 1,)),
            dma((3,)),
            dma((ne * nt - 1,)),
            dma((ne * nt - 1,)),
            dma((2, nt - 1)),
            dma((2, nt - 1)),
        ],
        compiler_params=pltpu.CompilerParams(collective_id=0, has_side_effects=True),
        name="moe_step",
    )(
        inputs_prev[0], cotangent_next[0], saved_input[0],
        *(lanes_last(v) for v in (expert_ids, keep_mask, slot_pos, weight_q)),
        gate_routed[0, 0], up_routed[0, 0], down_routed[0, 0],
        gate_shared[0], up_shared[0], down_shared[0],
    )
    return out[None], grad[None]


def solution(mesh):
    return jax.shard_map(
        local,
        mesh=mesh,
        in_specs=(
            P("pipe", "expert", "tensor"),
            P("pipe", "expert", "tensor"),
            P("pipe", "expert", "tensor"),
            P(None, "pipe", "expert", None),
            P(None, "pipe", "expert", None),
            P(None, "pipe", "expert", None),
            P(None, "pipe", "expert", None),
            P("pipe", "expert", None, "tensor"),
            P("pipe", "expert", None, "tensor"),
            P("pipe", "expert", "tensor", None),
            P("pipe", None, "tensor"),
            P("pipe", None, "tensor"),
            P("pipe", "tensor", None),
        ),
        out_specs=(P("pipe", "expert", "tensor"), P("pipe", "expert", "tensor")),
        check_vma=False,
    )
```
